1024 devices in a mesh: dp: 128 (over y, z), mp: 8 (over x, core).
Axes of the slice: x: 4, y: 4, z: 32, core: 2. Of those that a mesh axis runs over, the one named last changes fastest.
Arguments:
- tokens_in: bfloat16 [131072, 512], P('dp'), may hold values from -24 to 24
- out_grad: bfloat16 [131072, 8192], P('dp', 'mp'), may hold values from -0.015625 to 0.015625
- left_root: bfloat16 [512, 8192], P(None, 'mp'), may hold values from -1 to 31
- right_root: bfloat16 [512, 8192], P(None, 'mp'), may hold values from -1 to 31
- master: float32 [512, 8192], P('dp', 'mp'), may hold values from -3 to 3
Outputs:
- new_weight: float32 [512, 8192], P('dp', 'mp')
The draws below stay inside these ranges and needn't reach their ends.
All inputs are finite; a program needn't handle non-finite values.
Results may differ from the reference program's by a relative error of at most 0.0003.
Values sent between devices are 32-bit elements; how exact they have to be, the bound alone decides.
No kernel may reach another device: no remote copies, remote signals or barrier semaphores. Data moves between devices by JAX's collectives and lax.ppermute only.
A program may use at most 32 MiB of HBM per device.

```python
import jax
import jax.numpy as jnp
from jax import lax

BLOCK = 512
WIN_ROWS = 512
COLS = 8192
TOKENS = 131072


def block_factors(key):
    row_blocks = WIN_ROWS // BLOCK
    col_blocks = COLS // BLOCK
    noise_key, diag_key = jax.random.split(key)
    spread = 0.6 / jnp.sqrt(jnp.float32(BLOCK))
    offdiag = jnp.clip(jax.random.normal(noise_key, (row_blocks, BLOCK, col_blocks, BLOCK), jnp.float32), -4.0, 4.0) * spread
    logdiag = jax.random.uniform(diag_key, (row_blocks, BLOCK, col_blocks), jnp.float32, jnp.log(0.3), jnp.log(3.0))
    symmetric = 0.5 * (offdiag + jnp.transpose(offdiag, (0, 3, 2, 1)))
    identity = jnp.eye(BLOCK, dtype=jnp.float32)
    matrix = symmetric + jnp.exp(logdiag)[:, :, :, None] * identity[None, :, None, :]
    return matrix.reshape(WIN_ROWS, COLS)


def draw_left_root(key, part):
    return block_factors(jax.random.fold_in(key, 11)).astype(jnp.bfloat16)


def draw_right_root(key, part):
    return block_factors(jax.random.fold_in(key, 23)).astype(jnp.bfloat16)


def spiked(entries, stream_key, source, target, parts, factor):
    def block_of(position):
        return (jnp.arange(entries.shape[position]) // (entries.shape[position] // parts)).reshape((-1,) + (1,) * (entries.ndim - 1 - position))

    one_side = jax.random.permutation(stream_key, parts)[block_of(target)]
    far = (block_of(target) + parts // 2) % parts
    return jnp.where((block_of(source) == one_side) | (block_of(source) == far), factor * entries, entries)


def steps_of(rng, dims, pieces, low, top_value):
    def one(position, blocks):
        draws = jax.random.uniform(jax.random.fold_in(jax.random.fold_in(rng, 6), position), (blocks,), jnp.float32, low / len(pieces), top_value / len(pieces))
        return jnp.repeat(jnp.exp(draws), dims[position] // blocks).reshape((-1,) + (1,) * (len(dims) - position - 1))

    factor_of = one(*pieces[0])
    for cut in pieces[1:]:
        factor_of = factor_of * one(*cut)
    return factor_of


def scatter_about(own_key, shape, scale, limit, pieces=(), held_as=jnp.bfloat16):
    result = scale * jax.random.normal(own_key, shape, jnp.float32)
    if pieces:
        result = result * steps_of(own_key, shape, pieces, -0.22, 0.18)
    return jnp.clip(result, -limit, limit).astype(held_as)


def bell_draw_with(stream_key, dims, width, limit, shards, heavy, held_as=jnp.bfloat16):
    values = width * jax.random.normal(stream_key, dims, jnp.float32)
    if shards:
        values = values * steps_of(stream_key, dims, shards, -0.22, 0.18)
    return jnp.clip(spiked(values, jax.random.fold_in(stream_key, 3), *heavy), -limit, limit).astype(held_as)


def setup_inputs(seed: int = 0) -> dict:
    streams_of = jax.random.split(jax.random.key(seed), 6)
    tokens_in = bell_draw_with(streams_of[0], (TOKENS, WIN_ROWS), 1.0, 24.0, ((0, 128),), (0, 1, 128, 5.5))
    out_grad = scatter_about(streams_of[1], (TOKENS, COLS), TOKENS ** -0.5, 0.015625, ((0, 128), (1, 8)))
    left_root = draw_left_root(jax.random.fold_in(streams_of[5], 71), 0)
    right_root = draw_right_root(jax.random.fold_in(streams_of[5], 71), 0)
    master = scatter_about(streams_of[4], (WIN_ROWS, COLS), 0.5, 3.0, ((0, 128), (1, 8)), jnp.float32)
    return dict(tokens_in=tokens_in, out_grad=out_grad, left_root=left_root, right_root=right_root, master=master)


clip_rms = 10.0
step_size = 0.25
epsilon = 1e-06

def reference(tokens_in, out_grad, left_root, right_root, master):
    gradient = jnp.dot(tokens_in.T, out_grad, preferred_element_type=jnp.float32)
    row_blocks = WIN_ROWS // BLOCK
    col_blocks = COLS // BLOCK
    grad_blocks = gradient.reshape(row_blocks, BLOCK, col_blocks, BLOCK)
    left_full = left_root.astype(jnp.float32).reshape(row_blocks, BLOCK, col_blocks, BLOCK)
    right_full = right_root.astype(jnp.float32).reshape(row_blocks, BLOCK, col_blocks, BLOCK)
    left_mixed = jnp.einsum('irck,ikcj->ircj', left_full, grad_blocks, precision=lax.Precision.HIGHEST)
    precond = jnp.einsum('irck,ikcj->ircj', left_mixed, right_full, precision=lax.Precision.HIGHEST)
    precond = precond.reshape(WIN_ROWS, COLS)
    mean_square = jnp.sum(precond * precond) / jnp.float32(WIN_ROWS * COLS)
    root_mean = jnp.sqrt(mean_square + epsilon)
    factor = jnp.minimum(jnp.float32(1.0), clip_rms / root_mean)
    return master - step_size * factor * precond
```

```python
import jax
import jax.numpy as jnp
from jax import lax
from jax.experimental import pallas as pl
from jax.experimental.pallas import tpu as pltpu
from jax.sharding import Mesh
from jax.sharding import PartitionSpec as P

BLOCK = 512
Y, ZH, ZL, X, C = "dp_y", "dp_zh", "dp_zl", "mp_x", "mp_c"
DP = (Y, ZH, ZL)
MP = (X, C)
NY, NZH, NZL, NX, NC = 4, 16, 2, 4, 2
ROWS, COLS_DEV = 512, 1024
PEERS = NY * NX * NC
NZ = NZH * NZL
ENTRIES = 512 * 8192

clip_rms = 10.0
step_size = 0.25
epsilon = 1e-06

VMEM = pltpu.VMEM


def split(x):
    hi = x.astype(jnp.bfloat16)
    lo = (x - hi.astype(jnp.float32)).astype(jnp.bfloat16)
    return hi, lo


def dot(a, b):
    return jnp.dot(a, b, preferred_element_type=jnp.float32)


def grad_kernel(a_ref, b_ref, l_ref, o_ref):
    g = lax.dot_general(
        a_ref[...], b_ref[...], (((0,), (0,)), ((), ())), preferred_element_type=jnp.float32
    )
    hi, lo = split(g)
    left = l_ref[...]
    p = dot(left, hi) + dot(left, lo)
    o_ref[...] = p.reshape(NY, 1, ROWS // NY, BLOCK)


def mix_kernel(s_ref, r_ref, keep_ref, send_ref, ss_ref):
    zl = lax.axis_index(ZL)
    rows = jnp.sum(s_ref[...], axis=0)
    right = r_ref[:, pl.ds(pl.multiple_of(zl * BLOCK, BLOCK), BLOCK)]
    hi, lo = split(rows)
    p = dot(hi, right) + dot(lo, right)
    first, second = p[:4], p[4:]
    keep_ref[...] = jnp.where(zl == 0, first, second)
    send_ref[...] = jnp.where(zl == 0, second, first)
    sq = jnp.sum(p * p, axis=0, keepdims=True)
    part = sq[:, :128] + sq[:, 128:256] + sq[:, 256:384] + sq[:, 384:]
    ss_ref[...] = jnp.broadcast_to(part[None], ss_ref.shape)


def relay_kernel(s_ref, o_ref):
    o_ref[...] = jnp.broadcast_to(jnp.sum(s_ref[...], axis=0, keepdims=True), o_ref.shape)


def update_kernel(s_ref, m_ref, keep_ref, recv_ref, o_ref):
    zl = lax.axis_index(ZL)
    squares = jnp.sum(jnp.sum(s_ref[...], axis=0), axis=1, keepdims=True)
    root_mean = jnp.sqrt(squares / jnp.float32(ENTRIES) + epsilon)
    factor = jnp.minimum(jnp.float32(1.0), clip_rms / root_mean)
    scale = step_size * factor
    keep, recv = keep_ref[...], recv_ref[...]
    left = jnp.where(zl == 0, keep, recv)
    right = jnp.where(zl == 0, recv, keep)
    o_ref[:, :BLOCK] = m_ref[:, :BLOCK] - scale * left
    o_ref[:, BLOCK:] = m_ref[:, BLOCK:] - scale * right


def params(mib):
    return pltpu.CompilerParams(vmem_limit_bytes=mib * 1024 * 1024)


def whole(n):
    return [pl.BlockSpec(memory_space=VMEM)] * n


def f32(*shape):
    return jax.ShapeDtypeStruct(shape, jnp.float32)


def on_device(tokens_in, out_grad, left_root, right_root, master):
    partial = pl.pallas_call(
        grad_kernel,
        grid=(2,),
        in_specs=[
            pl.BlockSpec((1024, 512), lambda c: (0, 0)),
            pl.BlockSpec((1024, BLOCK), lambda c: (0, c)),
            pl.BlockSpec((BLOCK, BLOCK), lambda c: (0, c)),
        ],
        out_specs=pl.BlockSpec((NY, 1, ROWS // NY, BLOCK), lambda c: (0, c, 0, 0)),
        out_shape=f32(NY, NZL, ROWS // NY, BLOCK),
        compiler_params=params(24),
        name="grad",
    )(tokens_in, out_grad, left_root)
    terms = lax.all_to_all(
        partial.reshape(NY * NZL, ROWS // NY, BLOCK), (Y, ZL), 0, 0, tiled=True
    )
    rows = jnp.sum(terms, axis=0)
    terms = lax.all_to_all(rows.reshape(NZH, 8, BLOCK), ZH, 0, 0, tiled=True)
    keep, send, squares = pl.pallas_call(
        mix_kernel,
        in_specs=whole(2),
        out_specs=tuple(whole(3)),
        out_shape=(f32(4, BLOCK), f32(4, BLOCK), f32(PEERS, 1, 128)),
        compiler_params=params(8),
        name="mix",
    )(terms, right_root)
    recv = lax.ppermute(send, ZL, [(0, 1), (1, 0)])
    squares = lax.all_to_all(squares, (Y, X, C), 0, 0, tiled=True)
    squares = pl.pallas_call(
        relay_kernel,
        in_specs=whole(1),
        out_specs=pl.BlockSpec(memory_space=VMEM),
        out_shape=f32(NZ, 1, 128),
        compiler_params=params(4),
        name="relay",
    )(squares)
    squares = lax.all_to_all(squares, (ZH, ZL), 0, 0, tiled=True)
    return pl.pallas_call(
        update_kernel,
        in_specs=whole(4),
        out_specs=pl.BlockSpec(memory_space=VMEM),
        out_shape=f32(4, COLS_DEV),
        compiler_params=params(4),
        name="update",
    )(squares, master, keep, recv)


def solution(mesh):
    split_mesh = Mesh(mesh.devices.reshape(NY, NZH, NZL, NX, NC), (Y, ZH, ZL, X, C))
    in_specs = (P(DP, None), P(DP, MP), P(None, MP), P(None, MP), P(DP, MP))
    return jax.shard_map(
        on_device, mesh=split_mesh, in_specs=in_specs, out_specs=P(DP, MP), check_vma=False
    )
```

```python
import jax
import jax.numpy as jnp
from jax import lax
from jax.experimental import pallas as pl
from jax.experimental.pallas import tpu as pltpu
from jax.sharding import Mesh
from jax.sharding import PartitionSpec as P

BLOCK = 512
Y, ZH, ZL, X, C = "dp_y", "dp_zh", "dp_zl", "mp_x", "mp_c"
DP = (Y, ZH, ZL)
MP = (X, C)
NY, NZH, NZL, NX, NC = 4, 16, 2, 4, 2
ROWS, COLS_DEV = 512, 1024
PEERS = NY * NX * NC
NZ = NZH * NZL
ENTRIES = 512 * 8192

clip_rms = 10.0
step_size = 0.25
epsilon = 1e-06

VMEM = pltpu.VMEM


def split(x):
    hi = x.astype(jnp.bfloat16)
    lo = (x - hi.astype(jnp.float32)).astype(jnp.bfloat16)
    return hi, lo


def dot(a, b):
    return jnp.dot(a, b, preferred_element_type=jnp.float32)


def grad_kernel(a_hbm, b_hbm, l_hbm, o_ref, a_ref, b_ref, l_ref, sem):
    def columns(hbm, ref, c, k):
        return pltpu.make_async_copy(hbm.at[:, pl.ds(c * BLOCK, BLOCK)], ref.at[c], sem.at[k])

    tokens = pltpu.make_async_copy(a_hbm, a_ref, sem.at[0])
    grads = [columns(b_hbm, b_ref, c, 1 + c) for c in range(2)]
    lefts = [columns(l_hbm, l_ref, c, 3 + c) for c in range(2)]
    for copy in (tokens, grads[0], lefts[0], grads[1], lefts[1]):
        copy.start()
    tokens.wait()
    for c in range(2):
        grads[c].wait()
        g = lax.dot_general(
            a_ref[...], b_ref[c], (((0,), (0,)), ((), ())), preferred_element_type=jnp.float32
        )
        hi, lo = split(g)
        lefts[c].wait()
        left = l_ref[c]
        p = dot(left, hi) + dot(left, lo)
        o_ref[:, c] = p.reshape(NY, ROWS // NY, BLOCK)


def mix_kernel(s_ref, r_ref, keep_ref, send_ref, ss_ref):
    zl = lax.axis_index(ZL)
    rows = jnp.sum(s_ref[...], axis=0)
    right = r_ref[:, pl.ds(pl.multiple_of(zl * BLOCK, BLOCK), BLOCK)]
    hi, lo = split(rows)
    p = dot(hi, right) + dot(lo, right)
    first, second = p[:4], p[4:]
    keep_ref[...] = jnp.where(zl == 0, first, second)
    send_ref[...] = jnp.where(zl == 0, second, first)
    sq = jnp.sum(p * p, axis=0, keepdims=True)
    part = sq[:, :128] + sq[:, 128:256] + sq[:, 256:384] + sq[:, 384:]
    ss_ref[...] = jnp.broadcast_to(part[None], ss_ref.shape)


def relay_kernel(s_ref, o_ref):
    o_ref[...] = jnp.broadcast_to(jnp.sum(s_ref[...], axis=0, keepdims=True), o_ref.shape)


def update_kernel(s_ref, m_ref, keep_ref, recv_ref, o_ref):
    zl = lax.axis_index(ZL)
    squares = jnp.sum(jnp.sum(s_ref[...], axis=0), axis=1, keepdims=True)
    root_mean = jnp.sqrt(squares / jnp.float32(ENTRIES) + epsilon)
    factor = jnp.minimum(jnp.float32(1.0), clip_rms / root_mean)
    scale = step_size * factor
    keep, recv = keep_ref[...], recv_ref[...]
    left = jnp.where(zl == 0, keep, recv)
    right = jnp.where(zl == 0, recv, keep)
    o_ref[:, :BLOCK] = m_ref[:, :BLOCK] - scale * left
    o_ref[:, BLOCK:] = m_ref[:, BLOCK:] - scale * right


def params(mib):
    return pltpu.CompilerParams(vmem_limit_bytes=mib * 1024 * 1024)


def whole(n):
    return [pl.BlockSpec(memory_space=VMEM)] * n


def f32(*shape):
    return jax.ShapeDtypeStruct(shape, jnp.float32)


def on_device(tokens_in, out_grad, left_root, right_root, master):
    partial = pl.pallas_call(
        grad_kernel,
        in_specs=[pl.BlockSpec(memory_space=pltpu.HBM)] * 3,
        out_specs=pl.BlockSpec(memory_space=VMEM),
        out_shape=VMEM((NY, NZL, ROWS // NY, BLOCK), jnp.float32),
        scratch_shapes=[
            VMEM((1024, ROWS), jnp.bfloat16),
            VMEM((2, 1024, BLOCK), jnp.bfloat16),
            VMEM((2, BLOCK, BLOCK), jnp.bfloat16),
            pltpu.SemaphoreType.DMA((5,)),
        ],
        compiler_params=params(59),
        name="grad",
    )(tokens_in, out_grad, left_root)
    terms = lax.all_to_all(
        partial.reshape(NY * NZL, ROWS // NY, BLOCK), (Y, ZL), 0, 0, tiled=True
    )
    rows = jnp.sum(terms, axis=0)
    terms = lax.all_to_all(rows.reshape(NZH, 8, BLOCK), ZH, 0, 0, tiled=True)
    keep, send, squares = pl.pallas_call(
        mix_kernel,
        in_specs=whole(2),
        out_specs=tuple(whole(3)),
        out_shape=(f32(4, BLOCK), f32(4, BLOCK), f32(PEERS, 1, 128)),
        compiler_params=params(8),
        name="mix",
    )(terms, right_root)
    recv = lax.ppermute(send, ZL, [(0, 1), (1, 0)])
    squares = lax.all_to_all(squares, (Y, X, C), 0, 0, tiled=True)
    squares = pl.pallas_call(
        relay_kernel,
        in_specs=whole(1),
        out_specs=pl.BlockSpec(memory_space=VMEM),
        out_shape=VMEM((NZ, 1, 128), jnp.float32),
        compiler_params=params(4),
        name="relay",
    )(squares)
    squares = lax.all_to_all(squares, (ZH, ZL), 0, 0, tiled=True)
    return pl.pallas_call(
        update_kernel,
        in_specs=whole(4),
        out_specs=pl.BlockSpec(memory_space=VMEM),
        out_shape=f32(4, COLS_DEV),
        compiler_params=params(4),
        name="update",
    )(squares, master, keep, recv)


def solution(mesh):
    split_mesh = Mesh(mesh.devices.reshape(NY, NZH, NZL, NX, NC), (Y, ZH, ZL, X, C))
    in_specs = (P(DP, None), P(DP, MP), P(None, MP), P(None, MP), P(DP, MP))
    return jax.shard_map(
        on_device, mesh=split_mesh, in_specs=in_specs, out_specs=P(DP, MP), check_vma=False
    )
```

```python
import jax
import jax.numpy as jnp
from jax import lax
from jax.experimental import pallas as pl
from jax.experimental.pallas import tpu as pltpu
from jax.sharding import Mesh
from jax.sharding import PartitionSpec as P

BLOCK = 512
Y, ZH, ZM, ZL, X, C = "dp_y", "dp_zh", "dp_zm", "dp_zl", "mp_x", "mp_c"
DP = (Y, ZH, ZM, ZL)
MP = (X, C)
NY, NZH, NZM, NZL, NX, NC = 4, 8, 2, 2, 4, 2
ROWS, COLS_DEV = 512, 1024
PEERS = NY * NX * NC
NZ = NZH * NZM * NZL
ENTRIES = 512 * 8192

clip_rms = 10.0
step_size = 0.25
epsilon = 1e-06

VMEM = pltpu.VMEM


def split(x):
    hi = x.astype(jnp.bfloat16)
    lo = (x - hi.astype(jnp.float32)).astype(jnp.bfloat16)
    return hi, lo


def dot(a, b):
    return jnp.dot(a, b, preferred_element_type=jnp.float32)


def grad_kernel(a_hbm, b_hbm, l_hbm, o_ref, a_ref, b_ref, l_ref, sem):
    def columns(hbm, ref, c, k):
        return pltpu.make_async_copy(hbm.at[:, pl.ds(c * BLOCK, BLOCK)], ref.at[c], sem.at[k])

    tokens = pltpu.make_async_copy(a_hbm, a_ref, sem.at[0])
    grads = [columns(b_hbm, b_ref, c, 1 + c) for c in range(2)]
    lefts = [columns(l_hbm, l_ref, c, 3 + c) for c in range(2)]
    for copy in (tokens, grads[0], lefts[0], grads[1], lefts[1]):
        copy.start()
    tokens.wait()
    for c in range(2):
        grads[c].wait()
        g = lax.dot_general(
            a_ref[...], b_ref[c], (((0,), (0,)), ((), ())), preferred_element_type=jnp.float32
        )
        hi, lo = split(g)
        lefts[c].wait()
        left = l_ref[c]
        p = dot(left, hi) + dot(left, lo)
        p = p.reshape(NY, NZH, NZM, 8, BLOCK)
        for m in range(NZM):
            o_ref[:, c, m] = p[:, :, m]


def mix_kernel(s_ref, r_ref, keep_ref, send_ref, ss_ref):
    zl = lax.axis_index(ZL)
    rows = jnp.sum(s_ref[...], axis=0)
    right = r_ref[:, pl.ds(pl.multiple_of(zl * BLOCK, BLOCK), BLOCK)]
    hi, lo = split(rows)
    p = dot(hi, right) + dot(lo, right)
    first, second = p[:4], p[4:]
    keep_ref[...] = jnp.where(zl == 0, first, second)
    send_ref[...] = jnp.where(zl == 0, second, first)
    sq = jnp.sum(p * p, axis=0, keepdims=True)
    part = sq[:, :128] + sq[:, 128:256] + sq[:, 256:384] + sq[:, 384:]
    ss_ref[...] = jnp.broadcast_to(part[None], ss_ref.shape)


def relay_kernel(s_ref, o_ref):
    o_ref[...] = jnp.broadcast_to(jnp.sum(s_ref[...], axis=0, keepdims=True), o_ref.shape)


def update_kernel(s_ref, m_ref, keep_ref, recv_ref, o_ref):
    zl = lax.axis_index(ZL)
    squares = jnp.sum(jnp.sum(s_ref[...], axis=0), axis=1, keepdims=True)
    root_mean = jnp.sqrt(squares / jnp.float32(ENTRIES) + epsilon)
    factor = jnp.minimum(jnp.float32(1.0), clip_rms / root_mean)
    scale = step_size * factor
    keep, recv = keep_ref[...], recv_ref[...]
    left = jnp.where(zl == 0, keep, recv)
    right = jnp.where(zl == 0, recv, keep)
    o_ref[:, :BLOCK] = m_ref[:, :BLOCK] - scale * left
    o_ref[:, BLOCK:] = m_ref[:, BLOCK:] - scale * right


def params(mib):
    return pltpu.CompilerParams(vmem_limit_bytes=mib * 1024 * 1024)


def whole(n):
    return [pl.BlockSpec(memory_space=VMEM)] * n


def f32(*shape):
    return jax.ShapeDtypeStruct(shape, jnp.float32)


def on_device(tokens_in, out_grad, left_root, right_root, master):
    partial = pl.pallas_call(
        grad_kernel,
        in_specs=[pl.BlockSpec(memory_space=pltpu.HBM)] * 3,
        out_specs=pl.BlockSpec(memory_space=VMEM),
        out_shape=VMEM((NY, NZL, NZM, NZH, 8, BLOCK), jnp.float32),
        scratch_shapes=[
            VMEM((1024, ROWS), jnp.bfloat16),
            VMEM((2, 1024, BLOCK), jnp.bfloat16),
            VMEM((2, BLOCK, BLOCK), jnp.bfloat16),
            pltpu.SemaphoreType.DMA((5,)),
        ],
        compiler_params=params(59),
        name="grad",
    )(tokens_in, out_grad, left_root)
    terms = lax.all_to_all(
        partial.reshape(NY * NZL, ROWS // NY, BLOCK), (Y, ZL), 0, 0, tiled=True
    )
    rows = jnp.sum(terms, axis=0)
    terms = lax.all_to_all(rows.reshape(NZM, NZH * 8, BLOCK), ZM, 0, 0, tiled=True)
    rows = jnp.sum(terms, axis=0)
    terms = lax.all_to_all(rows.reshape(NZH, 8, BLOCK), ZH, 0, 0, tiled=True)
    keep, send, squares = pl.pallas_call(
        mix_kernel,
        in_specs=whole(2),
        out_specs=tuple(whole(3)),
        out_shape=(f32(4, BLOCK), f32(4, BLOCK), f32(PEERS, 1, 128)),
        compiler_params=params(8),
        name="mix",
    )(terms, right_root)
    recv = lax.ppermute(send, ZL, [(0, 1), (1, 0)])
    squares = lax.all_to_all(squares, (Y, X, C), 0, 0, tiled=True)
    squares = pl.pallas_call(
        relay_kernel,
        in_specs=whole(1),
        out_specs=pl.BlockSpec(memory_space=VMEM),
        out_shape=VMEM((NZ, 1, 128), jnp.float32),
        compiler_params=params(4),
        name="relay",
    )(squares)
    squares = lax.all_to_all(squares, (ZH, ZM, ZL), 0, 0, tiled=True)
    return pl.pallas_call(
        update_kernel,
        in_specs=whole(4),
        out_specs=pl.BlockSpec(memory_space=VMEM),
        out_shape=f32(4, COLS_DEV),
        compiler_params=params(4),
        name="update",
    )(squares, master, keep, recv)


def solution(mesh):
    split_mesh = Mesh(mesh.devices.reshape(NY, NZH, NZM, NZL, NX, NC), (Y, ZH, ZM, ZL, X, C))
    in_specs = (P(DP, None), P(DP, MP), P(None, MP), P(None, MP), P(DP, MP))
    return jax.shard_map(
        on_device, mesh=split_mesh, in_specs=in_specs, out_specs=P(DP, MP), check_vma=False
    )
```

```python
import jax
import jax.numpy as jnp
from jax import lax
from jax.experimental import pallas as pl
from jax.experimental.pallas import tpu as pltpu
from jax.sharding import Mesh
from jax.sharding import PartitionSpec as P

BLOCK = 512
Y, ZH, ZM, ZL, X, C = "dp_y", "dp_zh", "dp_zm", "dp_zl", "mp_x", "mp_c"
DP = (Y, ZH, ZM, ZL)
MP = (X, C)
NY, NZH, NZM, NZL, NX, NC = 4, 8, 2, 2, 4, 2
ROWS, COLS_DEV = 512, 1024
PEERS = NY * NX * NC
NEIGHBOURS = [
    [y * 32 + z % 32 for y in range(4) for z in ((2 * k + 1, 2 * k + 2) if k % 2 == 0 else (2 * k + 2, 2 * k + 1))]
    for k in range(16)
]
NZ = NZH * NZM * NZL
ENTRIES = 512 * 8192

clip_rms = 10.0
step_size = 0.25
epsilon = 1e-06

VMEM = pltpu.VMEM


def split(x):
    hi = x.astype(jnp.bfloat16)
    lo = (x - hi.astype(jnp.float32)).astype(jnp.bfloat16)
    return hi, lo


def dot(a, b):
    return jnp.dot(a, b, preferred_element_type=jnp.float32)


def grad_kernel(a_hbm, b_hbm, l_hbm, o_ref, a_ref, b_ref, l_ref, sem):
    def columns(hbm, ref, c, k):
        return pltpu.make_async_copy(hbm.at[:, pl.ds(c * BLOCK, BLOCK)], ref.at[c], sem.at[k])

    tokens = pltpu.make_async_copy(a_hbm, a_ref, sem.at[0])
    grads = [columns(b_hbm, b_ref, c, 1 + c) for c in range(2)]
    lefts = [columns(l_hbm, l_ref, c, 3 + c) for c in range(2)]
    for copy in (tokens, grads[0], lefts[0], grads[1], lefts[1]):
        copy.start()
    tokens.wait()
    for c in range(2):
        grads[c].wait()
        g = lax.dot_general(
            a_ref[...], b_ref[c], (((0,), (0,)), ((), ())), preferred_element_type=jnp.float32
        )
        hi, lo = split(g)
        lefts[c].wait()
        left = l_ref[c]
        p = dot(left, hi) + dot(left, lo)
        p = p.reshape(NY, NZH, NZM, 8, BLOCK)
        for m in range(NZM):
            o_ref[:, m, c] = p[:, :, m]


def mix_kernel(s_ref, r_ref, keep_ref, send_ref, ss_ref):
    zl = lax.axis_index(ZL)
    rows = jnp.sum(s_ref[...], axis=0)
    right = r_ref[:, pl.ds(pl.multiple_of(zl * BLOCK, BLOCK), BLOCK)]
    hi, lo = split(rows)
    p = dot(hi, right) + dot(lo, right)
    first, second = p[:4], p[4:]
    keep_ref[...] = jnp.where(zl == 0, first, second)
    send_ref[...] = jnp.where(zl == 0, second, first)
    sq = jnp.sum(p * p, axis=0, keepdims=True)
    part = sq[:, :128] + sq[:, 128:256] + sq[:, 256:384] + sq[:, 384:]
    ss_ref[...] = jnp.broadcast_to(part[None], ss_ref.shape)


def relay_kernel(s_ref, o_ref):
    o_ref[...] = jnp.broadcast_to(jnp.sum(s_ref[...], axis=0, keepdims=True), o_ref.shape)


def update_kernel(s_ref, m_ref, keep_ref, recv_ref, o_ref):
    zl = lax.axis_index(ZL)
    squares = jnp.sum(jnp.sum(s_ref[...], axis=0), axis=1, keepdims=True)
    root_mean = jnp.sqrt(squares / jnp.float32(ENTRIES) + epsilon)
    factor = jnp.minimum(jnp.float32(1.0), clip_rms / root_mean)
    scale = step_size * factor
    keep, recv = keep_ref[...], recv_ref[...]
    left = jnp.where(zl == 0, keep, recv)
    right = jnp.where(zl == 0, recv, keep)
    o_ref[:, :BLOCK] = m_ref[:, :BLOCK] - scale * left
    o_ref[:, BLOCK:] = m_ref[:, BLOCK:] - scale * right


def params(mib):
    return pltpu.CompilerParams(vmem_limit_bytes=mib * 1024 * 1024)


def whole(n):
    return [pl.BlockSpec(memory_space=VMEM)] * n


def f32(*shape):
    return jax.ShapeDtypeStruct(shape, jnp.float32)


def on_device(tokens_in, out_grad, left_root, right_root, master):
    partial = pl.pallas_call(
        grad_kernel,
        in_specs=[pl.BlockSpec(memory_space=pltpu.HBM)] * 3,
        out_specs=pl.BlockSpec(memory_space=VMEM),
        out_shape=VMEM((NY, NZM, NZL, NZH, 8, BLOCK), jnp.float32),
        scratch_shapes=[
            VMEM((1024, ROWS), jnp.bfloat16),
            VMEM((2, 1024, BLOCK), jnp.bfloat16),
            VMEM((2, BLOCK, BLOCK), jnp.bfloat16),
            pltpu.SemaphoreType.DMA((5,)),
        ],
        compiler_params=params(59),
        name="grad",
    )(tokens_in, out_grad, left_root)
    terms = lax.all_to_all(
        partial.reshape(NY * NZM, ROWS // NY, BLOCK),
        DP,
        0,
        0,
        axis_index_groups=NEIGHBOURS,
        tiled=True,
    )
    rows = jnp.sum(terms, axis=0)
    terms = lax.all_to_all(rows.reshape(NZL, NZH * 8, BLOCK), ZL, 0, 0, tiled=True)
    rows = jnp.sum(terms, axis=0)
    terms = lax.all_to_all(rows.reshape(NZH, 8, BLOCK), ZH, 0, 0, tiled=True)
    keep, send, squares = pl.pallas_call(
        mix_kernel,
        in_specs=whole(2),
        out_specs=tuple(whole(3)),
        out_shape=(f32(4, BLOCK), f32(4, BLOCK), f32(NZ, 1, 128)),
        compiler_params=params(8),
        name="mix",
    )(terms, right_root)
    recv = lax.ppermute(send, ZL, [(0, 1), (1, 0)])
    squares = lax.all_to_all(squares, (ZH, ZM, ZL), 0, 0, tiled=True)
    squares = pl.pallas_call(
        relay_kernel,
        in_specs=whole(1),
        out_specs=pl.BlockSpec(memory_space=VMEM),
        out_shape=VMEM((PEERS, 1, 128), jnp.float32),
        compiler_params=params(4),
        name="relay",
    )(squares)
    squares = lax.all_to_all(squares, (Y, X, C), 0, 0, tiled=True)
    return pl.pallas_call(
        update_kernel,
        in_specs=whole(4),
        out_specs=pl.BlockSpec(memory_space=VMEM),
        out_shape=f32(4, COLS_DEV),
        compiler_params=params(4),
        name="update",
    )(squares, master, keep, recv)


def solution(mesh):
    split_mesh = Mesh(mesh.devices.reshape(NY, NZH, NZM, NZL, NX, NC), (Y, ZH, ZM, ZL, X, C))
    in_specs = (P(DP, None), P(DP, MP), P(None, MP), P(None, MP), P(DP, MP))
    return jax.shard_map(
        on_device, mesh=split_mesh, in_specs=in_specs, out_specs=P(DP, MP), check_vma=False
    )
```

```python
import jax
import jax.numpy as jnp
from jax import lax
from jax.experimental import pallas as pl
from jax.experimental.pallas import tpu as pltpu
from jax.sharding import Mesh
from jax.sharding import PartitionSpec as P

BLOCK = 512
Y, ZH, ZM, ZL, X, C = "dp_y", "dp_zh", "dp_zm", "dp_zl", "mp_x", "mp_c"
DP = (Y, ZH, ZM, ZL)
MP = (X, C)
NY, NZH, NZM, NZL, NX, NC = 4, 8, 2, 2, 4, 2
ROWS, COLS_DEV = 512, 1024
PEERS = NY * NZM * NZL * NX * NC
NEIGHBOURS = [
    [y * 32 + z % 32 for y in range(4) for z in ((2 * k + 1, 2 * k + 2) if k % 2 == 0 else (2 * k + 2, 2 * k + 1))]
    for k in range(16)
]
ENTRIES = 512 * 8192

clip_rms = 10.0
step_size = 0.25
epsilon = 1e-06

VMEM = pltpu.VMEM


def split(x):
    hi = x.astype(jnp.bfloat16)
    lo = (x - hi.astype(jnp.float32)).astype(jnp.bfloat16)
    return hi, lo


def dot(a, b):
    return jnp.dot(a, b, preferred_element_type=jnp.float32)


def grad_kernel(a_hbm, b_hbm, l_hbm, o_ref, a_ref, b_ref, l_ref, sem):
    def columns(hbm, ref, c, k):
        return pltpu.make_async_copy(hbm.at[:, pl.ds(c * BLOCK, BLOCK)], ref.at[c], sem.at[k])

    tokens = pltpu.make_async_copy(a_hbm, a_ref, sem.at[0])
    grads = [columns(b_hbm, b_ref, c, 1 + c) for c in range(2)]
    lefts = [columns(l_hbm, l_ref, c, 3 + c) for c in range(2)]
    for copy in (tokens, grads[0], lefts[0], grads[1], lefts[1]):
        copy.start()
    tokens.wait()
    for c in range(2):
        grads[c].wait()
        g = lax.dot_general(
            a_ref[...], b_ref[c], (((0,), (0,)), ((), ())), preferred_element_type=jnp.float32
        )
        hi, lo = split(g)
        lefts[c].wait()
        left = l_ref[c]
        p = dot(left, hi) + dot(left, lo)
        p = p.reshape(NY, NZH, NZM, 8, BLOCK)
        for m in range(NZM):
            o_ref[:, m, :, :, pl.ds(c * BLOCK, BLOCK)] = p[:, :, m]


def fold_kernel(s_ref, o_ref):
    rows = jnp.sum(s_ref[...], axis=0)
    o_ref[0] = rows[:, :4]
    o_ref[1] = rows[:, 4:]


def mix_kernel(s_ref, r_ref, p_ref, ss_ref):
    rows = jnp.sum(s_ref[...], axis=0)
    hi, lo = split(rows)
    total = jnp.zeros((1, 128), jnp.float32)
    for c in range(2):
        cols = pl.ds(c * BLOCK, BLOCK)
        right = r_ref[:, cols]
        here = slice(c * BLOCK, (c + 1) * BLOCK)
        p = dot(hi[:, here], right) + dot(lo[:, here], right)
        p_ref[:, cols] = p
        sq = jnp.sum(p * p, axis=0, keepdims=True)
        total = total + (sq[:, :128] + sq[:, 128:256] + sq[:, 256:384] + sq[:, 384:])
    ss_ref[...] = jnp.broadcast_to(total[None], ss_ref.shape)


def relay_kernel(s_ref, o_ref):
    o_ref[...] = jnp.sum(s_ref[...], axis=0)


def update_kernel(s_ref, m_ref, p_ref, o_ref):
    squares = jnp.sum(jnp.sum(s_ref[...], axis=0), axis=1, keepdims=True)
    root_mean = jnp.sqrt(squares / jnp.float32(ENTRIES) + epsilon)
    factor = jnp.minimum(jnp.float32(1.0), clip_rms / root_mean)
    scale = step_size * factor
    o_ref[...] = m_ref[...] - scale * p_ref[...]


def params(mib):
    return pltpu.CompilerParams(vmem_limit_bytes=mib * 1024 * 1024)


def whole(n):
    return [pl.BlockSpec(memory_space=VMEM)] * n


def f32(*shape):
    return jax.ShapeDtypeStruct(shape, jnp.float32)


def on_device(tokens_in, out_grad, left_root, right_root, master):
    partial = pl.pallas_call(
        grad_kernel,
        in_specs=[pl.BlockSpec(memory_space=pltpu.HBM)] * 3,
        out_specs=pl.BlockSpec(memory_space=VMEM),
        out_shape=VMEM((NY, NZM, NZH, 8, COLS_DEV), jnp.float32),
        scratch_shapes=[
            VMEM((1024, ROWS), jnp.bfloat16),
            VMEM((2, 1024, BLOCK), jnp.bfloat16),
            VMEM((2, BLOCK, BLOCK), jnp.bfloat16),
            pltpu.SemaphoreType.DMA((5,)),
        ],
        compiler_params=params(59),
        name="grad",
    )(tokens_in, out_grad, left_root)
    terms = lax.all_to_all(
        partial.reshape(NY * NZM, NZH, 8, COLS_DEV),
        DP,
        0,
        0,
        axis_index_groups=NEIGHBOURS,
        tiled=True,
    )
    rows = pl.pallas_call(
        fold_kernel,
        in_specs=whole(1),
        out_specs=pl.BlockSpec(memory_space=VMEM),
        out_shape=VMEM((NZL, NZH, 4, COLS_DEV), jnp.float32),
        compiler_params=params(8),
        name="fold",
    )(terms)
    terms = lax.all_to_all(rows, ZL, 0, 0, tiled=True)
    rows = jnp.sum(terms, axis=0)
    terms = lax.all_to_all(rows, ZH, 0, 0, tiled=True)
    precond, squares = pl.pallas_call(
        mix_kernel,
        in_specs=whole(2),
        out_specs=tuple(whole(2)),
        out_shape=(f32(4, COLS_DEV), VMEM((PEERS, 1, 128), jnp.float32)),
        compiler_params=params(8),
        name="mix",
    )(terms, right_root)
    squares = lax.all_to_all(squares, (Y, ZM, ZL, X, C), 0, 0, tiled=True)
    squares = pl.pallas_call(
        relay_kernel,
        in_specs=whole(1),
        out_specs=pl.BlockSpec(memory_space=VMEM),
        out_shape=VMEM((1, 128), jnp.float32),
        compiler_params=params(4),
        name="relay",
    )(squares)
    squares = lax.all_gather(squares, ZH)
    return pl.pallas_call(
        update_kernel,
        in_specs=whole(3),
        out_specs=pl.BlockSpec(memory_space=VMEM),
        out_shape=f32(4, COLS_DEV),
        compiler_params=params(4),
        name="update",
    )(squares, master, precond)


def solution(mesh):
    split_mesh = Mesh(mesh.devices.reshape(NY, NZH, NZM, NZL, NX, NC), (Y, ZH, ZM, ZL, X, C))
    in_specs = (P(DP, None), P(DP, MP), P(None, MP), P(None, MP), P(DP, MP))
    return jax.shard_map(
        on_device, mesh=split_mesh, in_specs=in_specs, out_specs=P(DP, MP), check_vma=False
    )
```

```python
import jax
import jax.numpy as jnp
from jax import lax
from jax.experimental import pallas as pl
from jax.experimental.pallas import tpu as pltpu
from jax.sharding import Mesh
from jax.sharding import PartitionSpec as P

BLOCK = 512
Y, ZH, ZM, ZL, X, C = "dp_y", "dp_zh", "dp_zm", "dp_zl", "mp_x", "mp_c"
DP = (Y, ZH, ZM, ZL)
MP = (X, C)
NY, NZH, NZM, NZL, NX, NC = 4, 8, 2, 2, 4, 2
ROWS, COLS_DEV = 512, 1024
PEERS = NY * NZM * NZL * NX * NC
NEIGHBOURS = [
    [y * 32 + z % 32 for y in range(4) for z in ((2 * k + 1, 2 * k + 2) if k % 2 == 0 else (2 * k + 2, 2 * k + 1))]
    for k in range(16)
]
ENTRIES = 512 * 8192


def rank(y, z, x, c):
    return ((y * 32 + z) * NX + x) * NC + c


GATHERS = [
    [rank(y, r + 4 * q, x, 1) for q in range(8)] for y in range(4) for x in range(4) for r in range(4)
] + [
    [rank(y, z + (i ^ y) % 2, x, 0) for y in range(4) for i in range(2)]
    for z in range(0, 32, 2)
    for x in range(4)
]

clip_rms = 10.0
step_size = 0.25
epsilon = 1e-06

VMEM = pltpu.VMEM


def split(x):
    hi = x.astype(jnp.bfloat16)
    lo = (x - hi.astype(jnp.float32)).astype(jnp.bfloat16)
    return hi, lo


def dot(a, b):
    return jnp.dot(a, b, preferred_element_type=jnp.float32)


def grad_kernel(a_hbm, b_hbm, l_hbm, o_ref, a_ref, b_ref, l_ref, sem):
    def columns(hbm, ref, c, k):
        return pltpu.make_async_copy(hbm.at[:, pl.ds(c * BLOCK, BLOCK)], ref.at[c], sem.at[k])

    tokens = pltpu.make_async_copy(a_hbm, a_ref, sem.at[0])
    grads = [columns(b_hbm, b_ref, c, 1 + c) for c in range(2)]
    lefts = [columns(l_hbm, l_ref, c, 3 + c) for c in range(2)]
    for copy in (tokens, grads[0], lefts[0], grads[1], lefts[1]):
        copy.start()
    tokens.wait()
    for c in range(2):
        grads[c].wait()
        g = lax.dot_general(
            a_ref[...], b_ref[c], (((0,), (0,)), ((), ())), preferred_element_type=jnp.float32
        )
        hi, lo = split(g)
        lefts[c].wait()
        left = l_ref[c]
        p = dot(left, hi) + dot(left, lo)
        p = p.reshape(NY, NZH, NZM, 8, BLOCK)
        for m in range(NZM):
            o_ref[:, m, :, :, pl.ds(c * BLOCK, BLOCK)] = p[:, :, m]


def fold_kernel(s_ref, o_ref):
    rows = jnp.sum(s_ref[...], axis=0)
    o_ref[0] = rows[:, :4]
    o_ref[1] = rows[:, 4:]


def mix_kernel(s_ref, r_ref, p_ref, ss_ref):
    rows = jnp.sum(s_ref[...], axis=0)
    hi, lo = split(rows)
    total = jnp.zeros((1, 128), jnp.float32)
    for c in range(2):
        cols = pl.ds(c * BLOCK, BLOCK)
        right = r_ref[:, cols]
        here = slice(c * BLOCK, (c + 1) * BLOCK)
        p = dot(hi[:, here], right) + dot(lo[:, here], right)
        p_ref[:, cols] = p
        sq = jnp.sum(p * p, axis=0, keepdims=True)
        total = total + (sq[:, :128] + sq[:, 128:256] + sq[:, 256:384] + sq[:, 384:])
    ss_ref[...] = jnp.broadcast_to(total[None], ss_ref.shape)


def relay_kernel(s_ref, o_ref):
    o_ref[...] = jnp.sum(s_ref[...], axis=0)


def update_kernel(s_ref, t_ref, m_ref, p_ref, o_ref):
    squares = jnp.where(lax.axis_index(C) == 1, s_ref[...], t_ref[...])
    squares = jnp.sum(jnp.sum(squares, axis=0), axis=1, keepdims=True)
    root_mean = jnp.sqrt(squares / jnp.float32(ENTRIES) + epsilon)
    factor = jnp.minimum(jnp.float32(1.0), clip_rms / root_mean)
    scale = step_size * factor
    o_ref[...] = m_ref[...] - scale * p_ref[...]


def params(mib):
    return pltpu.CompilerParams(vmem_limit_bytes=mib * 1024 * 1024)


def whole(n):
    return [pl.BlockSpec(memory_space=VMEM)] * n


def f32(*shape):
    return jax.ShapeDtypeStruct(shape, jnp.float32)


def on_device(tokens_in, out_grad, left_root, right_root, master):
    partial = pl.pallas_call(
        grad_kernel,
        in_specs=[pl.BlockSpec(memory_space=pltpu.HBM)] * 3,
        out_specs=pl.BlockSpec(memory_space=VMEM),
        out_shape=VMEM((NY, NZM, NZH, 8, COLS_DEV), jnp.float32),
        scratch_shapes=[
            VMEM((1024, ROWS), jnp.bfloat16),
            VMEM((2, 1024, BLOCK), jnp.bfloat16),
            VMEM((2, BLOCK, BLOCK), jnp.bfloat16),
            pltpu.SemaphoreType.DMA((5,)),
        ],
        compiler_params=params(59),
        name="grad",
    )(tokens_in, out_grad, left_root)
    terms = lax.all_to_all(
        partial.reshape(NY * NZM, NZH, 8, COLS_DEV),
        DP,
        0,
        0,
        axis_index_groups=NEIGHBOURS,
        tiled=True,
    )
    rows = pl.pallas_call(
        fold_kernel,
        in_specs=whole(1),
        out_specs=pl.BlockSpec(memory_space=VMEM),
        out_shape=VMEM((NZL, NZH, 4, COLS_DEV), jnp.float32),
        compiler_params=params(8),
        name="fold",
    )(terms)
    terms = lax.all_to_all(rows, ZL, 0, 0, tiled=True)
    rows = jnp.sum(terms, axis=0)
    terms = lax.all_to_all(rows, ZH, 0, 0, tiled=True)
    precond, squares = pl.pallas_call(
        mix_kernel,
        in_specs=whole(2),
        out_specs=tuple(whole(2)),
        out_shape=(f32(4, COLS_DEV), VMEM((PEERS, 1, 128), jnp.float32)),
        compiler_params=params(8),
        name="mix",
    )(terms, right_root)
    squares = lax.all_to_all(squares, (Y, ZM, ZL, X, C), 0, 0, tiled=True)
    squares = pl.pallas_call(
        relay_kernel,
        in_specs=whole(1),
        out_specs=pl.BlockSpec(memory_space=VMEM),
        out_shape=VMEM((1, 128), jnp.float32),
        compiler_params=params(4),
        name="relay",
    )(squares)
    squares = lax.all_gather(squares, DP + MP, axis_index_groups=GATHERS)
    across = lax.ppermute(squares, C, [(1, 0)])
    return pl.pallas_call(
        update_kernel,
        in_specs=whole(4),
        out_specs=pl.BlockSpec(memory_space=VMEM),
        out_shape=f32(4, COLS_DEV),
        compiler_params=params(4),
        name="update",
    )(squares, across, master, precond)


def solution(mesh):
    split_mesh = Mesh(mesh.devices.reshape(NY, NZH, NZM, NZL, NX, NC), (Y, ZH, ZM, ZL, X, C))
    in_specs = (P(DP, None), P(DP, MP), P(None, MP), P(None, MP), P(DP, MP))
    return jax.shard_map(
        on_device, mesh=split_mesh, in_specs=in_specs, out_specs=P(DP, MP), check_vma=False
    )
```

```python
import jax
import jax.numpy as jnp
from jax import lax
from jax.experimental import pallas as pl
from jax.experimental.pallas import tpu as pltpu
from jax.sharding import Mesh
from jax.sharding import PartitionSpec as P

BLOCK = 512
Y, ZH, ZM, ZL, X, C = "dp_y", "dp_zh", "dp_zm", "dp_zl", "mp_x", "mp_c"
DP = (Y, ZH, ZM, ZL)
MP = (X, C)
NY, NZH, NZM, NZL, NX, NC = 4, 8, 2, 2, 4, 2
ROWS, COLS_DEV = 512, 1024
PEERS = NY * NZM * NZL * NX * NC
def gray(z):
    return (z ^ z >> 1) & 1


def bit1(z):
    return z >> 1 & 1


FIRST = [
    [y * 32 + z for y in range(NY) for z in sorted((2 * j, 2 * j + 1), key=gray)] for j in range(16)
]
SECOND = [
    [y * 32 + z for z in sorted((2 * k + 1, (2 * k + 2) % 32), key=bit1)]
    for y in range(NY)
    for k in range(16)
]
ENTRIES = 512 * 8192


def rank(y, z, x, c):
    return ((y * 32 + z) * NX + x) * NC + c


GATHERS = [
    [rank(y, r + 4 * q, x, 1) for q in range(8)] for y in range(4) for x in range(4) for r in range(4)
] + [
    [rank(y, z + (i ^ y) % 2, x, 0) for y in range(4) for i in range(2)]
    for z in range(0, 32, 2)
    for x in range(4)
]

clip_rms = 10.0
step_size = 0.25
epsilon = 1e-06

VMEM = pltpu.VMEM


def split(x):
    hi = x.astype(jnp.bfloat16)
    lo = (x - hi.astype(jnp.float32)).astype(jnp.bfloat16)
    return hi, lo


def dot(a, b):
    return jnp.dot(a, b, preferred_element_type=jnp.float32)


def grad_kernel(a_hbm, b_hbm, l_hbm, o_ref, a_ref, b_ref, l_ref, sem):
    def columns(hbm, ref, c, k):
        return pltpu.make_async_copy(hbm.at[:, pl.ds(c * BLOCK, BLOCK)], ref.at[c], sem.at[k])

    tokens = pltpu.make_async_copy(a_hbm, a_ref, sem.at[0])
    grads = [columns(b_hbm, b_ref, c, 1 + c) for c in range(2)]
    lefts = [columns(l_hbm, l_ref, c, 3 + c) for c in range(2)]
    for copy in (tokens, grads[0], lefts[0], grads[1], lefts[1]):
        copy.start()
    tokens.wait()
    for c in range(2):
        grads[c].wait()
        g = lax.dot_general(
            a_ref[...], b_ref[c], (((0,), (0,)), ((), ())), preferred_element_type=jnp.float32
        )
        hi, lo = split(g)
        lefts[c].wait()
        left = l_ref[c]
        p = dot(left, hi) + dot(left, lo)
        p = p.reshape(NY, NZH, NZM, 8, BLOCK)
        even, odd = p[:, :, 0], p[:, :, 1]
        upper = lax.broadcasted_iota(jnp.int32, even.shape, 2) < 4
        cols = pl.ds(c * BLOCK, BLOCK)
        o_ref[:, 0, :, :, cols] = jnp.where(upper, even, odd)
        o_ref[:, 1, :, :, cols] = jnp.where(upper, odd, even)


def fold_kernel(s_ref, o_ref):
    rows = jnp.sum(s_ref[...], axis=0)
    same = lax.axis_index(ZM) == lax.axis_index(ZL)
    o_ref[0] = jnp.where(same, rows[:, :4], rows[:, 4:])
    o_ref[1] = jnp.where(same, rows[:, 4:], rows[:, :4])


def mix_kernel(s_ref, r_ref, p_ref, ss_ref):
    rows = jnp.sum(s_ref[...], axis=0)
    hi, lo = split(rows)
    total = jnp.zeros((1, 128), jnp.float32)
    for c in range(2):
        cols = pl.ds(c * BLOCK, BLOCK)
        right = r_ref[:, cols]
        here = slice(c * BLOCK, (c + 1) * BLOCK)
        p = dot(hi[:, here], right) + dot(lo[:, here], right)
        p_ref[:, cols] = p
        sq = jnp.sum(p * p, axis=0, keepdims=True)
        total = total + (sq[:, :128] + sq[:, 128:256] + sq[:, 256:384] + sq[:, 384:])
    ss_ref[...] = jnp.broadcast_to(total[None], ss_ref.shape)


def relay_kernel(s_ref, o_ref):
    o_ref[...] = jnp.sum(s_ref[...], axis=0)


def update_kernel(s_ref, t_ref, m_ref, p_ref, o_ref):
    squares = jnp.where(lax.axis_index(C) == 1, s_ref[...], t_ref[...])
    squares = jnp.sum(jnp.sum(squares, axis=0), axis=1, keepdims=True)
    root_mean = jnp.sqrt(squares / jnp.float32(ENTRIES) + epsilon)
    factor = jnp.minimum(jnp.float32(1.0), clip_rms / root_mean)
    scale = step_size * factor
    o_ref[...] = m_ref[...] - scale * p_ref[...]


def params(mib):
    return pltpu.CompilerParams(vmem_limit_bytes=mib * 1024 * 1024)


def whole(n):
    return [pl.BlockSpec(memory_space=VMEM)] * n


def f32(*shape):
    return jax.ShapeDtypeStruct(shape, jnp.float32)


def on_device(tokens_in, out_grad, left_root, right_root, master):
    partial = pl.pallas_call(
        grad_kernel,
        in_specs=[pl.BlockSpec(memory_space=pltpu.HBM)] * 3,
        out_specs=pl.BlockSpec(memory_space=VMEM),
        out_shape=VMEM((NY, 2, NZH, 8, COLS_DEV), jnp.float32),
        scratch_shapes=[
            VMEM((1024, ROWS), jnp.bfloat16),
            VMEM((2, 1024, BLOCK), jnp.bfloat16),
            VMEM((2, BLOCK, BLOCK), jnp.bfloat16),
            pltpu.SemaphoreType.DMA((5,)),
        ],
        compiler_params=params(59),
        name="grad",
    )(tokens_in, out_grad, left_root)
    terms = lax.all_to_all(
        partial.reshape(NY * 2, NZH, 8, COLS_DEV),
        DP,
        0,
        0,
        axis_index_groups=FIRST,
        tiled=True,
    )
    rows = pl.pallas_call(
        fold_kernel,
        in_specs=whole(1),
        out_specs=pl.BlockSpec(memory_space=VMEM),
        out_shape=VMEM((NZM, NZH, 4, COLS_DEV), jnp.float32),
        compiler_params=params(8),
        name="fold",
    )(terms)
    terms = lax.all_to_all(rows, DP, 0, 0, axis_index_groups=SECOND, tiled=True)
    rows = jnp.sum(terms, axis=0)
    terms = lax.all_to_all(rows, ZH, 0, 0, tiled=True)
    precond, squares = pl.pallas_call(
        mix_kernel,
        in_specs=whole(2),
        out_specs=tuple(whole(2)),
        out_shape=(f32(4, COLS_DEV), VMEM((PEERS, 1, 128), jnp.float32)),
        compiler_params=params(8),
        name="mix",
    )(terms, right_root)
    squares = lax.all_to_all(squares, (Y, ZM, ZL, X, C), 0, 0, tiled=True)
    squares = pl.pallas_call(
        relay_kernel,
        in_specs=whole(1),
        out_specs=pl.BlockSpec(memory_space=VMEM),
        out_shape=VMEM((1, 128), jnp.float32),
        compiler_params=params(4),
        name="relay",
    )(squares)
    squares = lax.all_gather(squares, DP + MP, axis_index_groups=GATHERS)
    across = lax.ppermute(squares, C, [(1, 0)])
    return pl.pallas_call(
        update_kernel,
        in_specs=whole(4),
        out_specs=pl.BlockSpec(memory_space=VMEM),
        out_shape=f32(4, COLS_DEV),
        compiler_params=params(4),
        name="update",
    )(squares, across, master, precond)


def solution(mesh):
    split_mesh = Mesh(mesh.devices.reshape(NY, NZH, NZM, NZL, NX, NC), (Y, ZH, ZM, ZL, X, C))
    in_specs = (P(DP, None), P(DP, MP), P(None, MP), P(None, MP), P(DP, MP))
    return jax.shard_map(
        on_device, mesh=split_mesh, in_specs=in_specs, out_specs=P(DP, MP), check_vma=False
    )
```

```python
import jax
import jax.numpy as jnp
from jax import lax
from jax.experimental import pallas as pl
from jax.experimental.pallas import tpu as pltpu
from jax.sharding import Mesh
from jax.sharding import PartitionSpec as P

BLOCK = 512
Y, ZH, ZM, ZL, X, C = "dp_y", "dp_zh", "dp_zm", "dp_zl", "mp_x", "mp_c"
DP = (Y, ZH, ZM, ZL)
MP = (X, C)
NY, NZH, NZM, NZL, NX, NC = 4, 8, 2, 2, 4, 2
ROWS, COLS_DEV = 512, 1024
PEERS = NY * NZM * NZL * NX * NC
def gray(z):
    return (z ^ z >> 1) & 1


def bit1(z):
    return z >> 1 & 1


FIRST = [
    [y * 32 + z for y in range(NY) for z in sorted((2 * j, 2 * j + 1), key=gray)] for j in range(16)
]
SECOND = [
    [y * 32 + z for z in sorted((2 * k + 1, (2 * k + 2) % 32), key=bit1)]
    for y in range(NY)
    for k in range(16)
]
ENTRIES = 512 * 8192
LEAD_NS = 8000


def rank(y, z, x, c):
    return ((y * 32 + z) * NX + x) * NC + c


GATHERS = [
    [rank(y, r + 4 * q, x, 1) for q in range(8)] for y in range(4) for x in range(4) for r in range(4)
] + [
    [rank(y, z + (i ^ y) % 2, x, 0) for y in range(4) for i in range(2)]
    for z in range(0, 32, 2)
    for x in range(4)
]

clip_rms = 10.0
step_size = 0.25
epsilon = 1e-06

VMEM = pltpu.VMEM


def split(x):
    hi = x.astype(jnp.bfloat16)
    lo = (x - hi.astype(jnp.float32)).astype(jnp.bfloat16)
    return hi, lo


def dot(a, b):
    return jnp.dot(a, b, preferred_element_type=jnp.float32)


def grad_kernel(a_hbm, b_hbm, l_hbm, o_ref, a_ref, b_ref, l_ref, sem):
    def columns(hbm, ref, c, k):
        return pltpu.make_async_copy(hbm.at[:, pl.ds(c * BLOCK, BLOCK)], ref.at[c], sem.at[k])

    tokens = pltpu.make_async_copy(a_hbm, a_ref, sem.at[0])
    grads = [columns(b_hbm, b_ref, c, 1 + c) for c in range(2)]
    lefts = [columns(l_hbm, l_ref, c, 3 + c) for c in range(2)]
    for copy in (tokens, grads[0], lefts[0], grads[1], lefts[1]):
        copy.start()
    tokens.wait()
    for c in range(2):
        grads[c].wait()
        g = lax.dot_general(
            a_ref[...], b_ref[c], (((0,), (0,)), ((), ())), preferred_element_type=jnp.float32
        )
        hi, lo = split(g)
        lefts[c].wait()
        left = l_ref[c]
        p = dot(left, hi) + dot(left, lo)
        p = p.reshape(NY, NZH, NZM, 8, BLOCK)
        even, odd = p[:, :, 0], p[:, :, 1]
        upper = lax.broadcasted_iota(jnp.int32, even.shape, 2) < 4
        cols = pl.ds(c * BLOCK, BLOCK)
        o_ref[:, 0, :, :, cols] = jnp.where(upper, even, odd)
        o_ref[:, 1, :, :, cols] = jnp.where(upper, odd, even)

    @pl.when(lax.axis_index(C) == 1)
    def _():
        pl.delay(LEAD_NS)


def fold_kernel(s_ref, o_ref):
    rows = jnp.sum(s_ref[...], axis=0)
    same = lax.axis_index(ZM) == lax.axis_index(ZL)
    o_ref[0] = jnp.where(same, rows[:, :4], rows[:, 4:])
    o_ref[1] = jnp.where(same, rows[:, 4:], rows[:, :4])


def mix_kernel(s_ref, r_ref, p_ref, ss_ref):
    rows = jnp.sum(s_ref[...], axis=0)
    hi, lo = split(rows)
    total = jnp.zeros((1, 128), jnp.float32)
    for c in range(2):
        cols = pl.ds(c * BLOCK, BLOCK)
        right = r_ref[:, cols]
        here = slice(c * BLOCK, (c + 1) * BLOCK)
        p = dot(hi[:, here], right) + dot(lo[:, here], right)
        p_ref[:, cols] = p
        sq = jnp.sum(p * p, axis=0, keepdims=True)
        total = total + (sq[:, :128] + sq[:, 128:256] + sq[:, 256:384] + sq[:, 384:])
    ss_ref[...] = jnp.broadcast_to(total[None], ss_ref.shape)


def relay_kernel(s_ref, o_ref):
    o_ref[...] = jnp.sum(s_ref[...], axis=0)


def update_kernel(s_ref, t_ref, m_ref, p_ref, o_ref):
    squares = jnp.where(lax.axis_index(C) == 1, s_ref[...], t_ref[...])
    squares = jnp.sum(jnp.sum(squares, axis=0), axis=1, keepdims=True)
    root_mean = jnp.sqrt(squares / jnp.float32(ENTRIES) + epsilon)
    factor = jnp.minimum(jnp.float32(1.0), clip_rms / root_mean)
    scale = step_size * factor
    o_ref[...] = m_ref[...] - scale * p_ref[...]


def params(mib):
    return pltpu.CompilerParams(vmem_limit_bytes=mib * 1024 * 1024)


def whole(n):
    return [pl.BlockSpec(memory_space=VMEM)] * n


def f32(*shape):
    return jax.ShapeDtypeStruct(shape, jnp.float32)


def on_device(tokens_in, out_grad, left_root, right_root, master):
    partial = pl.pallas_call(
        grad_kernel,
        in_specs=[pl.BlockSpec(memory_space=pltpu.HBM)] * 3,
        out_specs=pl.BlockSpec(memory_space=VMEM),
        out_shape=VMEM((NY, 2, NZH, 8, COLS_DEV), jnp.float32),
        scratch_shapes=[
            VMEM((1024, ROWS), jnp.bfloat16),
            VMEM((2, 1024, BLOCK), jnp.bfloat16),
            VMEM((2, BLOCK, BLOCK), jnp.bfloat16),
            pltpu.SemaphoreType.DMA((5,)),
        ],
        compiler_params=params(59),
        name="grad",
    )(tokens_in, out_grad, left_root)
    terms = lax.all_to_all(
        partial.reshape(NY * 2, NZH, 8, COLS_DEV),
        DP,
        0,
        0,
        axis_index_groups=FIRST,
        tiled=True,
    )
    rows = pl.pallas_call(
        fold_kernel,
        in_specs=whole(1),
        out_specs=pl.BlockSpec(memory_space=VMEM),
        out_shape=VMEM((NZM, NZH, 4, COLS_DEV), jnp.float32),
        compiler_params=params(8),
        name="fold",
    )(terms)
    terms = lax.all_to_all(rows, DP, 0, 0, axis_index_groups=SECOND, tiled=True)
    rows = jnp.sum(terms, axis=0)
    terms = lax.all_to_all(rows, ZH, 0, 0, tiled=True)
    precond, squares = pl.pallas_call(
        mix_kernel,
        in_specs=whole(2),
        out_specs=tuple(whole(2)),
        out_shape=(f32(4, COLS_DEV), VMEM((PEERS, 1, 128), jnp.float32)),
        compiler_params=params(8),
        name="mix",
    )(terms, right_root)
    squares = lax.all_to_all(squares, (Y, ZM, ZL, X, C), 0, 0, tiled=True)
    squares = pl.pallas_call(
        relay_kernel,
        in_specs=whole(1),
        out_specs=pl.BlockSpec(memory_space=VMEM),
        out_shape=VMEM((1, 128), jnp.float32),
        compiler_params=params(4),
        name="relay",
    )(squares)
    squares = lax.all_gather(squares, DP + MP, axis_index_groups=GATHERS)
    across = lax.ppermute(squares, C, [(1, 0)])
    return pl.pallas_call(
        update_kernel,
        in_specs=whole(4),
        out_specs=pl.BlockSpec(memory_space=VMEM),
        out_shape=f32(4, COLS_DEV),
        compiler_params=params(4),
        name="update",
    )(squares, across, master, precond)


def solution(mesh):
    split_mesh = Mesh(mesh.devices.reshape(NY, NZH, NZM, NZL, NX, NC), (Y, ZH, ZM, ZL, X, C))
    in_specs = (P(DP, None), P(DP, MP), P(None, MP), P(None, MP), P(DP, MP))
    return jax.shard_map(
        on_device, mesh=split_mesh, in_specs=in_specs, out_specs=P(DP, MP), check_vma=False
    )
```

```python
import jax
import jax.numpy as jnp
from jax import lax
from jax.experimental import pallas as pl
from jax.experimental.pallas import tpu as pltpu
from jax.sharding import Mesh
from jax.sharding import PartitionSpec as P

BLOCK = 512
Y, ZH, ZM, ZL, X, C = "dp_y", "dp_zh", "dp_zm", "dp_zl", "mp_x", "mp_c"
DP = (Y, ZH, ZM, ZL)
MP = (X, C)
NY, NZH, NZM, NZL, NX, NC = 4, 8, 2, 2, 4, 2
ROWS, COLS_DEV = 512, 1024
PEERS = NY * NZM * NZL * NX * NC
def gray(z):
    return (z ^ z >> 1) & 1


def bit1(z):
    return z >> 1 & 1


FIRST = [
    [y * 32 + z for y in range(NY) for z in sorted((2 * j, 2 * j + 1), key=gray)] for j in range(16)
]
SECOND = [
    [y * 32 + z for z in sorted((2 * k + 1, (2 * k + 2) % 32), key=bit1)]
    for y in range(NY)
    for k in range(16)
]
ENTRIES = 512 * 8192
LEAD_NS = 5500


def rank(y, z, x, c):
    return ((y * 32 + z) * NX + x) * NC + c


GATHERS = [
    [rank(y, r + 4 * q, x, 1) for q in range(8)] for y in range(4) for x in range(4) for r in range(4)
] + [
    [rank(y, z + (i ^ y) % 2, x, 0) for y in range(4) for i in range(2)]
    for z in range(0, 32, 2)
    for x in range(4)
]

clip_rms = 10.0
step_size = 0.25
epsilon = 1e-06

VMEM = pltpu.VMEM


def split(x):
    hi = x.astype(jnp.bfloat16)
    lo = (x - hi.astype(jnp.float32)).astype(jnp.bfloat16)
    return hi, lo


def dot(a, b):
    return jnp.dot(a, b, preferred_element_type=jnp.float32)


def grad_kernel(a_hbm, b_hbm, l_hbm, o_ref, a_ref, b_ref, l_ref, sem):
    def columns(hbm, ref, c, k):
        return pltpu.make_async_copy(hbm.at[:, pl.ds(c * BLOCK, BLOCK)], ref.at[c], sem.at[k])

    tokens = pltpu.make_async_copy(a_hbm, a_ref, sem.at[0])
    grads = [columns(b_hbm, b_ref, c, 1 + c) for c in range(2)]
    lefts = [columns(l_hbm, l_ref, c, 3 + c) for c in range(2)]
    for copy in (tokens, grads[0], lefts[0], grads[1], lefts[1]):
        copy.start()
    tokens.wait()
    for c in range(2):
        grads[c].wait()
        g = lax.dot_general(
            a_ref[...], b_ref[c], (((0,), (0,)), ((), ())), preferred_element_type=jnp.float32
        )
        hi, lo = split(g)
        lefts[c].wait()
        left = l_ref[c]
        p = dot(left, hi) + dot(left, lo)
        p = p.reshape(NY, NZH, NZM, 8, BLOCK)
        even, odd = p[:, :, 0], p[:, :, 1]
        upper = lax.broadcasted_iota(jnp.int32, even.shape, 2) < 4
        cols = pl.ds(c * BLOCK, BLOCK)
        o_ref[:, 0, :, :, cols] = jnp.where(upper, even, odd)
        o_ref[:, 1, :, :, cols] = jnp.where(upper, odd, even)

    @pl.when(lax.axis_index(C) == 1)
    def _():
        pl.delay(LEAD_NS)


def fold_kernel(s_ref, o_ref):
    rows = jnp.sum(s_ref[...], axis=0)
    same = lax.axis_index(ZM) == lax.axis_index(ZL)
    o_ref[0] = jnp.where(same, rows[:, :4], rows[:, 4:])
    o_ref[1] = jnp.where(same, rows[:, 4:], rows[:, :4])


def mix_kernel(s_ref, r_ref, p_ref, ss_ref):
    rows = jnp.sum(s_ref[...], axis=0)
    hi, lo = split(rows)
    total = jnp.zeros((1, 128), jnp.float32)
    for c in range(2):
        cols = pl.ds(c * BLOCK, BLOCK)
        right = r_ref[:, cols]
        here = slice(c * BLOCK, (c + 1) * BLOCK)
        p = dot(hi[:, here], right) + dot(lo[:, here], right)
        p_ref[:, cols] = p
        sq = jnp.sum(p * p, axis=0, keepdims=True)
        total = total + (sq[:, :128] + sq[:, 128:256] + sq[:, 256:384] + sq[:, 384:])
    ss_ref[...] = jnp.broadcast_to(total[None], ss_ref.shape)


def relay_kernel(s_ref, o_ref):
    o_ref[...] = jnp.sum(s_ref[...], axis=0)


def update_kernel(s_ref, t_ref, m_ref, p_ref, o_ref):
    squares = jnp.where(lax.axis_index(C) == 1, s_ref[...], t_ref[...])
    squares = jnp.sum(jnp.sum(squares, axis=0), axis=1, keepdims=True)
    root_mean = jnp.sqrt(squares / jnp.float32(ENTRIES) + epsilon)
    factor = jnp.minimum(jnp.float32(1.0), clip_rms / root_mean)
    scale = step_size * factor
    o_ref[...] = m_ref[...] - scale * p_ref[...]


def params(mib):
    return pltpu.CompilerParams(vmem_limit_bytes=mib * 1024 * 1024)


def whole(n):
    return [pl.BlockSpec(memory_space=VMEM)] * n


def f32(*shape):
    return jax.ShapeDtypeStruct(shape, jnp.float32)


def on_device(tokens_in, out_grad, left_root, right_root, master):
    partial = pl.pallas_call(
        grad_kernel,
        in_specs=[pl.BlockSpec(memory_space=pltpu.HBM)] * 3,
        out_specs=pl.BlockSpec(memory_space=VMEM),
        out_shape=VMEM((NY, 2, NZH, 8, COLS_DEV), jnp.float32),
        scratch_shapes=[
            VMEM((1024, ROWS), jnp.bfloat16),
            VMEM((2, 1024, BLOCK), jnp.bfloat16),
            VMEM((2, BLOCK, BLOCK), jnp.bfloat16),
            pltpu.SemaphoreType.DMA((5,)),
        ],
        compiler_params=params(59),
        name="grad",
    )(tokens_in, out_grad, left_root)
    terms = lax.all_to_all(
        partial.reshape(NY * 2, NZH, 8, COLS_DEV),
        DP,
        0,
        0,
        axis_index_groups=FIRST,
        tiled=True,
    )
    rows = pl.pallas_call(
        fold_kernel,
        in_specs=whole(1),
        out_specs=pl.BlockSpec(memory_space=VMEM),
        out_shape=VMEM((NZM, NZH, 4, COLS_DEV), jnp.float32),
        compiler_params=params(8),
        name="fold",
    )(terms)
    terms = lax.all_to_all(rows, DP, 0, 0, axis_index_groups=SECOND, tiled=True)
    rows = jnp.sum(terms, axis=0)
    terms = lax.all_to_all(rows, ZH, 0, 0, tiled=True)
    precond, squares = pl.pallas_call(
        mix_kernel,
        in_specs=whole(2),
        out_specs=tuple(whole(2)),
        out_shape=(f32(4, COLS_DEV), VMEM((PEERS, 1, 128), jnp.float32)),
        compiler_params=params(8),
        name="mix",
    )(terms, right_root)
    squares = lax.all_to_all(squares, (Y, ZM, ZL, X, C), 0, 0, tiled=True)
    squares = pl.pallas_call(
        relay_kernel,
        in_specs=whole(1),
        out_specs=pl.BlockSpec(memory_space=VMEM),
        out_shape=VMEM((1, 128), jnp.float32),
        compiler_params=params(4),
        name="relay",
    )(squares)
    squares = lax.all_gather(squares, DP + MP, axis_index_groups=GATHERS)
    across = lax.ppermute(squares, C, [(1, 0)])
    return pl.pallas_call(
        update_kernel,
        in_specs=whole(4),
        out_specs=pl.BlockSpec(memory_space=VMEM),
        out_shape=f32(4, COLS_DEV),
        compiler_params=params(4),
        name="update",
    )(squares, across, master, precond)


def solution(mesh):
    split_mesh = Mesh(mesh.devices.reshape(NY, NZH, NZM, NZL, NX, NC), (Y, ZH, ZM, ZL, X, C))
    in_specs = (P(DP, None), P(DP, MP), P(None, MP), P(None, MP), P(DP, MP))
    return jax.shard_map(
        on_device, mesh=split_mesh, in_specs=in_specs, out_specs=P(DP, MP), check_vma=False
    )
```

```python
import jax
import jax.numpy as jnp
from jax import lax
from jax.experimental import pallas as pl
from jax.experimental.pallas import tpu as pltpu
from jax.sharding import Mesh
from jax.sharding import PartitionSpec as P

BLOCK = 512
Y, ZH, ZM, ZL, X, C = "dp_y", "dp_zh", "dp_zm", "dp_zl", "mp_x", "mp_c"
DP = (Y, ZH, ZM, ZL)
MP = (X, C)
NY, NZH, NZM, NZL, NX, NC = 4, 8, 2, 2, 4, 2
ROWS, COLS_DEV = 512, 1024
PEERS = NY * NZM * NZL * NX * NC
def gray(z):
    return (z ^ z >> 1) & 1


def bit1(z):
    return z >> 1 & 1


FIRST = [
    [y * 32 + z for y in range(NY) for z in sorted((2 * j, 2 * j + 1), key=gray)] for j in range(16)
]
SECOND = [
    [y * 32 + z for z in sorted((2 * k + 1, (2 * k + 2) % 32), key=bit1)]
    for y in range(NY)
    for k in range(16)
]
ENTRIES = 512 * 8192
LEAD_NS = 9500


def rank(y, z, x, c):
    return ((y * 32 + z) * NX + x) * NC + c


GATHERS = [
    [rank(y, r + 4 * q, x, 1) for q in range(8)] for y in range(4) for x in range(4) for r in range(4)
] + [
    [rank(y, z + (i ^ y) % 2, x, 0) for y in range(4) for i in range(2)]
    for z in range(0, 32, 2)
    for x in range(4)
]

clip_rms = 10.0
step_size = 0.25
epsilon = 1e-06

VMEM = pltpu.VMEM


def split(x):
    hi = x.astype(jnp.bfloat16)
    lo = (x - hi.astype(jnp.float32)).astype(jnp.bfloat16)
    return hi, lo


def dot(a, b):
    return jnp.dot(a, b, preferred_element_type=jnp.float32)


def grad_kernel(a_hbm, b_hbm, l_hbm, o_ref, a_ref, b_ref, l_ref, sem):
    def columns(hbm, ref, c, k):
        return pltpu.make_async_copy(hbm.at[:, pl.ds(c * BLOCK, BLOCK)], ref.at[c], sem.at[k])

    tokens = pltpu.make_async_copy(a_hbm, a_ref, sem.at[0])
    grads = [columns(b_hbm, b_ref, c, 1 + c) for c in range(2)]
    lefts = [columns(l_hbm, l_ref, c, 3 + c) for c in range(2)]
    for copy in (tokens, grads[0], lefts[0], grads[1], lefts[1]):
        copy.start()
    tokens.wait()
    for c in range(2):
        grads[c].wait()
        g = lax.dot_general(
            a_ref[...], b_ref[c], (((0,), (0,)), ((), ())), preferred_element_type=jnp.float32
        )
        hi, lo = split(g)
        lefts[c].wait()
        left = l_ref[c]
        p = dot(left, hi) + dot(left, lo)
        p = p.reshape(NY, NZH, NZM, 8, BLOCK)
        even, odd = p[:, :, 0], p[:, :, 1]
        upper = lax.broadcasted_iota(jnp.int32, even.shape, 2) < 4
        cols = pl.ds(c * BLOCK, BLOCK)
        o_ref[:, 0, :, :, cols] = jnp.where(upper, even, odd)
        o_ref[:, 1, :, :, cols] = jnp.where(upper, odd, even)

    @pl.when(lax.axis_index(C) == 1)
    def _():
        pl.delay(LEAD_NS)


def fold_kernel(s_ref, o_ref):
    rows = jnp.sum(s_ref[...], axis=0)
    same = lax.axis_index(ZM) == lax.axis_index(ZL)
    o_ref[0] = jnp.where(same, rows[:, :4], rows[:, 4:])
    o_ref[1] = jnp.where(same, rows[:, 4:], rows[:, :4])


def mix_kernel(s_ref, r_ref, p_ref, ss_ref):
    rows = jnp.sum(s_ref[...], axis=0)
    hi, lo = split(rows)
    total = jnp.zeros((1, 128), jnp.float32)
    for c in range(2):
        cols = pl.ds(c * BLOCK, BLOCK)
        right = r_ref[:, cols]
        here = slice(c * BLOCK, (c + 1) * BLOCK)
        p = dot(hi[:, here], right) + dot(lo[:, here], right)
        p_ref[:, cols] = p
        sq = jnp.sum(p * p, axis=0, keepdims=True)
        total = total + (sq[:, :128] + sq[:, 128:256] + sq[:, 256:384] + sq[:, 384:])
    ss_ref[...] = jnp.broadcast_to(total[None], ss_ref.shape)


def relay_kernel(s_ref, o_ref):
    o_ref[...] = jnp.sum(s_ref[...], axis=0)


def update_kernel(s_ref, t_ref, m_ref, p_ref, o_ref):
    squares = jnp.where(lax.axis_index(C) == 1, s_ref[...], t_ref[...])
    squares = jnp.sum(jnp.sum(squares, axis=0), axis=1, keepdims=True)
    root_mean = jnp.sqrt(squares / jnp.float32(ENTRIES) + epsilon)
    factor = jnp.minimum(jnp.float32(1.0), clip_rms / root_mean)
    scale = step_size * factor
    o_ref[...] = m_ref[...] - scale * p_ref[...]


def params(mib):
    return pltpu.CompilerParams(vmem_limit_bytes=mib * 1024 * 1024)


def whole(n):
    return [pl.BlockSpec(memory_space=VMEM)] * n


def f32(*shape):
    return jax.ShapeDtypeStruct(shape, jnp.float32)


def on_device(tokens_in, out_grad, left_root, right_root, master):
    partial = pl.pallas_call(
        grad_kernel,
        in_specs=[pl.BlockSpec(memory_space=pltpu.HBM)] * 3,
        out_specs=pl.BlockSpec(memory_space=VMEM),
        out_shape=VMEM((NY, 2, NZH, 8, COLS_DEV), jnp.float32),
        scratch_shapes=[
            VMEM((1024, ROWS), jnp.bfloat16),
            VMEM((2, 1024, BLOCK), jnp.bfloat16),
            VMEM((2, BLOCK, BLOCK), jnp.bfloat16),
            pltpu.SemaphoreType.DMA((5,)),
        ],
        compiler_params=params(59),
        name="grad",
    )(tokens_in, out_grad, left_root)
    terms = lax.all_to_all(
        partial.reshape(NY * 2, NZH, 8, COLS_DEV),
        DP,
        0,
        0,
        axis_index_groups=FIRST,
        tiled=True,
    )
    rows = pl.pallas_call(
        fold_kernel,
        in_specs=whole(1),
        out_specs=pl.BlockSpec(memory_space=VMEM),
        out_shape=VMEM((NZM, NZH, 4, COLS_DEV), jnp.float32),
        compiler_params=params(8),
        name="fold",
    )(terms)
    terms = lax.all_to_all(rows, DP, 0, 0, axis_index_groups=SECOND, tiled=True)
    rows = jnp.sum(terms, axis=0)
    terms = lax.all_to_all(rows, ZH, 0, 0, tiled=True)
    precond, squares = pl.pallas_call(
        mix_kernel,
        in_specs=whole(2),
        out_specs=tuple(whole(2)),
        out_shape=(f32(4, COLS_DEV), VMEM((PEERS, 1, 128), jnp.float32)),
        compiler_params=params(8),
        name="mix",
    )(terms, right_root)
    squares = lax.all_to_all(squares, (Y, ZM, ZL, X, C), 0, 0, tiled=True)
    squares = pl.pallas_call(
        relay_kernel,
        in_specs=whole(1),
        out_specs=pl.BlockSpec(memory_space=VMEM),
        out_shape=VMEM((1, 128), jnp.float32),
        compiler_params=params(4),
        name="relay",
    )(squares)
    squares = lax.all_gather(squares, DP + MP, axis_index_groups=GATHERS)
    across = lax.ppermute(squares, C, [(1, 0)])
    return pl.pallas_call(
        update_kernel,
        in_specs=whole(4),
        out_specs=pl.BlockSpec(memory_space=VMEM),
        out_shape=f32(4, COLS_DEV),
        compiler_params=params(4),
        name="update",
    )(squares, across, master, precond)


def solution(mesh):
    split_mesh = Mesh(mesh.devices.reshape(NY, NZH, NZM, NZL, NX, NC), (Y, ZH, ZM, ZL, X, C))
    in_specs = (P(DP, None), P(DP, MP), P(None, MP), P(None, MP), P(DP, MP))
    return jax.shard_map(
        on_device, mesh=split_mesh, in_specs=in_specs, out_specs=P(DP, MP), check_vma=False
    )
```
